32 devices in a mesh: vocab: 8 (over z, y), batch: 4 (over x, core).
Axes of the slice: x: 2, y: 2, z: 4, core: 2. Of those that a mesh axis runs over, the one named last changes fastest.
Arguments:
- latent_state_rows: bfloat16 [64, 8192], P('batch', 'vocab'), may hold values from -90 to 90
- closing_rescale_coeffs: bfloat16 [8192], replicated, may hold values from 0.5 to 1.5
- output_projection_matrix: bfloat16 [8192, 131072], P(None, ('vocab', 'batch')), may hold values from -3.7565048 to 3.7565048
- config_heat_values: float32 [16], replicated, may hold values from 0.7 to 1.4
- sequence_config_choice: int32 [64], replicated, may hold values from 0 to 15
- ranked_choice_ids: int32 [64, 128], replicated, may hold values from 0 to 131071
- keep_count: int32 [64], replicated, may hold values from 2 to 128
Outputs:
- log_norm: float32 [64], P('batch')
- kept_mass: float32 [64], P('batch')
- renormed: float32 [64, 128], P('batch')
The draws below stay inside these ranges and needn't reach their ends.
All inputs are finite; a program needn't handle non-finite values.
Results may differ from the reference program's by a relative error of at most 0.0048.
Values may be sent and summed in bfloat16 or wider, within the bound.
No kernel may reach another device: no remote copies, remote signals or barrier semaphores. Data moves between devices by JAX's collectives and lax.ppermute only.
A program may use at most 128 MiB of HBM per device.

```python
import math
import jax
import jax.numpy as jnp
from jax import lax

D = 8192
VOCAB = 131072
CAND = 128
SAMPLER_CONFIGS = 16
SG = 16
SLOTS = 64
N_VOCAB = 8
N_BATCH = 4


def weight_block(key, block):
    return jnp.clip(jax.random.normal(jax.random.fold_in(jax.random.fold_in(key, 11), block), (D, 128), jnp.float32), -5.0, 5.0)


def column_scale(key):
    position = jnp.arange(VOCAB, dtype=jnp.float32) / VOCAB
    spread = jnp.exp(jax.random.uniform(jax.random.fold_in(key, 12), (VOCAB,), jnp.float32, math.log(0.45), math.log(2.2)))
    trend = 0.75 + 0.5 * position
    return 2.0 * spread * trend


def drawn_pairs():
    pairs = []
    targets = [160.0, 200.0, 240.0, 160.0, 200.0, 240.0]
    for number in range(6):
        first_id = (5003 + 24011 * number) % VOCAB
        second_id = (first_id + 7) % VOCAB
        row_index = number * SLOTS // 6
        pairs.append((first_id, second_id, row_index, targets[number]))
    return pairs


def draw_output_projection_matrix(key, part):
    blocks = jax.vmap(lambda block: weight_block(key, block), out_axes=1)(jnp.arange(VOCAB // 128))
    matrix = blocks.reshape(D, VOCAB) * (column_scale(key) / math.sqrt(D))[None, :]
    return matrix.astype(jnp.bfloat16)


def draw_latent_state_rows(key, part):
    values = jnp.clip(jax.random.normal(jax.random.fold_in(key, 13), (SLOTS, D), jnp.float32), -5.0, 5.0)
    return values.astype(jnp.bfloat16)


def draw_ranked_choice_ids(key, part):
    ids = jax.random.randint(jax.random.fold_in(key, 16), (SLOTS, CAND), 0, VOCAB, jnp.int32)
    shard_count = N_VOCAB * N_BATCH
    shard_width = VOCAB // shard_count
    group_of = jnp.arange(SLOTS, dtype=jnp.int32) // SG
    offsets = jax.random.randint(jax.random.fold_in(key, 17), (SLOTS, 2), 0, shard_width, jnp.int32)
    near_shard = (group_of + 1) % shard_count
    far_shard = (group_of + shard_count // 2) % shard_count
    ids = ids.at[:, 0].set(near_shard * shard_width + offsets[:, 0])
    ids = ids.at[:, 1].set(far_shard * shard_width + offsets[:, 1])
    for first_id, second_id, row_index, target in drawn_pairs():
        ids = ids.at[row_index, 0].set(jnp.int32(first_id))
        ids = ids.at[row_index, 1].set(jnp.int32(second_id))
    return ids


def touch_ends(values, own_key, low, top_value):
    extent = values.shape
    place = [jax.random.randint(jax.random.fold_in(own_key, axis), (), 0, extent[axis]) for axis in range(len(extent))]
    values = values.at[tuple(place)].set(low)
    longest = extent.index(max(extent))
    place[longest] = (place[longest] + 1) % extent[longest]
    return values.at[tuple(place)].set(top_value)


def setup_inputs(seed: int = 0) -> dict:
    key_list = jax.random.split(jax.random.key(seed), 8)
    latent_state_rows = draw_latent_state_rows(jax.random.fold_in(key_list[7], 71), 0)
    closing_rescale_coeffs = jnp.clip(1.0 + 0.1 * jax.random.normal(key_list[1], (D,), jnp.float32), 0.5, 1.5).astype(jnp.bfloat16)
    output_projection_matrix = draw_output_projection_matrix(jax.random.fold_in(key_list[7], 71), 0)
    config_heat_values = jnp.clip(jnp.exp(jax.random.uniform(key_list[3], (SAMPLER_CONFIGS,), jnp.float32, math.log(0.7), math.log(1.4))), 0.7, 1.4)
    sequence_config_choice = touch_ends(jax.random.randint(key_list[4], (SLOTS,), 0, SAMPLER_CONFIGS), jax.random.fold_in(key_list[4], 1), 0, SAMPLER_CONFIGS - 1).astype(jnp.int32)
    ranked_choice_ids = draw_ranked_choice_ids(jax.random.fold_in(key_list[7], 71), 0)
    keep_count = touch_ends(jax.random.randint(key_list[6], (SLOTS,), 2, CAND + 1), jax.random.fold_in(key_list[6], 1), 2, CAND).astype(jnp.int32)
    return {"latent_state_rows": latent_state_rows, "closing_rescale_coeffs": closing_rescale_coeffs, "output_projection_matrix": output_projection_matrix, "config_heat_values": config_heat_values, "sequence_config_choice": sequence_config_choice, "ranked_choice_ids": ranked_choice_ids, "keep_count": keep_count}


epsilon = 1e-06

def reference(latent_state_rows, closing_rescale_coeffs, output_projection_matrix, config_heat_values, sequence_config_choice, ranked_choice_ids, keep_count):
    values = latent_state_rows.astype(jnp.float32)
    mean_square = lax.optimization_barrier(jnp.mean(values * values, axis=1, keepdims=True))
    normed = (values * lax.rsqrt(mean_square + epsilon) * closing_rescale_coeffs.astype(jnp.float32)[None, :]).astype(jnp.bfloat16)
    unnormalized_scores = jnp.dot(normed, output_projection_matrix, preferred_element_type=jnp.float32)
    config_membership = (sequence_config_choice[:, None] == jnp.arange(SAMPLER_CONFIGS, dtype=jnp.int32)[None, :]).astype(jnp.float32)
    sequence_heat_values = lax.optimization_barrier(jnp.sum(config_membership * config_heat_values[None, :], axis=1))
    divided_scores = unnormalized_scores / sequence_heat_values[:, None]
    row_top = lax.optimization_barrier(jnp.max(divided_scores, axis=1))
    row_total = lax.optimization_barrier(jnp.sum(jnp.exp(divided_scores - row_top[:, None]), axis=1))
    log_norm = row_top + jnp.log(row_total)
    picked = jnp.take_along_axis(divided_scores, ranked_choice_ids.astype(jnp.int32), axis=1)
    kept_mask = jnp.arange(CAND, dtype=jnp.int32)[None, :] < keep_count[:, None]
    kept_top = lax.optimization_barrier(jnp.max(jnp.where(kept_mask, picked, jnp.float32(-3e+38)), axis=1))
    shifted = jnp.where(kept_mask, picked - kept_top[:, None], jnp.float32(0.0))
    kept_exp = jnp.where(kept_mask, jnp.exp(shifted), jnp.float32(0.0))
    kept_sum = lax.optimization_barrier(jnp.sum(kept_exp, axis=1))
    kept_mass = kept_top + jnp.log(kept_sum) - log_norm
    return (log_norm, kept_mass, kept_exp / kept_sum[:, None])
```

```python
import functools

import jax
import jax.numpy as jnp
from jax import lax
from jax.experimental import pallas as pl
from jax.experimental.pallas import tpu as pltpu
from jax.sharding import PartitionSpec as P


epsilon = 1e-06
LANES = 128
UNITS = 32
CHUNKS = 2
EARLY_UNITS = (6, 4, 5, 1)
BESIDE_UNITS = 6
MIB = 1 << 20
SLAB = 1024


VMEM = pl.BlockSpec(memory_space=pltpu.VMEM)
SMEM = pl.BlockSpec(memory_space=pltpu.SMEM)
ANY = pl.BlockSpec(memory_space=pl.ANY)


def bits_of(count):
    return [1 << n for n in range(count.bit_length() - 1)]


def swap(value, axis, bit):
    count = lax.axis_size(axis)
    return lax.ppermute(value, axis, [(n, n ^ bit) for n in range(count)])


def swap_both(value, vocab_offset, batch_offset):
    vocab_count = lax.axis_size("vocab")
    batch_count = lax.axis_size("batch")
    pairs = [
        (v * batch_count + b, (v ^ vocab_offset) * batch_count + (b ^ batch_offset))
        for v in range(vocab_count)
        for b in range(batch_count)
    ]
    return lax.ppermute(value, ("vocab", "batch"), pairs)


def rounds_of(bits):
    bits = sorted(bits, reverse=True)
    return [bits[n : n + 2] for n in range(0, len(bits), 2)]


def offsets_of(bits):
    offsets = [0]
    for bit in bits:
        offsets += [offset ^ bit for offset in offsets]
    return offsets


def unit_copies(span, matrix_ref, target_ref, sems):
    first, count = span
    height = target_ref.shape[0] // count
    return [
        pltpu.make_async_copy(
            matrix_ref.at[pl.ds((first + n) * height, height)],
            target_ref.at[pl.ds(n * height, height)],
            sems.at[n],
        )
        for n in range(count)
    ]


def fetch_kernel(*refs, span):
    matrix_ref, out_ref, sems = refs[-3:]
    copies = unit_copies(span, matrix_ref, out_ref, sems)
    for copy in copies:
        copy.start()
    for copy in copies:
        copy.wait()


def rows_shape(span, matrix):
    features, cols = matrix.shape
    return pltpu.VMEM((features // UNITS * span[1], cols), matrix.dtype)


def fetch(span, matrix, after=None):
    operands = [matrix] if after is None else [after, matrix]
    return pl.pallas_call(
        functools.partial(fetch_kernel, span=span),
        out_shape=rows_shape(span, matrix),
        in_specs=[ANY] * len(operands),
        out_specs=VMEM,
        scratch_shapes=[pltpu.SemaphoreType.DMA((span[1],))],
        compiler_params=pltpu.CompilerParams(vmem_limit_bytes=MIB),
        cost_estimate=pl.CostEstimate(
            flops=span[1] * 10**10, bytes_accessed=matrix.size * 2 // UNITS * span[1], transcendentals=0
        ),
    )(*operands)


def norm_kernel(pieces_ref, gain_ref, *out_refs, offsets):
    vocab_pos = lax.axis_index("vocab")
    count, group_rows, part = pieces_ref.shape
    per_chunk = count // CHUNKS
    order_bits = [offsets[1 << n] for n in range(count.bit_length() - 1)]
    square = jnp.zeros((group_rows, part), jnp.float32)
    for n in range(count):
        values = pieces_ref[n].astype(jnp.float32)
        square = square + values * values
    factor = lax.rsqrt(jnp.sum(square, axis=1, keepdims=True) / (count * part) + epsilon)
    for n in range(count):
        apart = vocab_pos ^ n
        place = sum(
            ((apart >> (bit.bit_length() - 1)) & 1) << k for k, bit in enumerate(order_bits)
        )
        values = pieces_ref[place].astype(jnp.float32)
        gain = gain_ref[n * part : (n + 1) * part].astype(jnp.float32).reshape(1, part)
        out_refs[n // per_chunk][0, :, pl.ds(n % per_chunk * part, part)] = (
            values * factor * gain
        ).astype(jnp.bfloat16)


def norm(pieces, gain, offsets):
    count, group_rows, part = pieces.shape
    chunk = jax.ShapeDtypeStruct((1, group_rows, count * part // CHUNKS), jnp.bfloat16)
    return pl.pallas_call(
        functools.partial(norm_kernel, offsets=offsets),
        out_shape=(chunk,) * CHUNKS,
        in_specs=[VMEM, VMEM],
        out_specs=(VMEM,) * CHUNKS,
        compiler_params=pltpu.CompilerParams(vmem_limit_bytes=4 * MIB),
        name="norm",
    )(pieces, gain)


def product(rows_ref, chunk, weight_ref, span, cols, total=None):
    groups, group_rows, width = rows_ref.shape
    per_chunk = UNITS // CHUNKS
    unit = width // per_chunk
    low = max(span[0], chunk * per_chunk)
    high = min(span[0] + span[1], (chunk + 1) * per_chunk)
    if low >= high:
        return total
    rows = rows_ref[
        :, :, (low - chunk * per_chunk) * unit : (high - chunk * per_chunk) * unit
    ].reshape(groups * group_rows, (high - low) * unit)
    weights = weight_ref[(low - span[0]) * unit : (high - span[0]) * unit, cols]
    term = jnp.dot(rows, weights, preferred_element_type=jnp.float32)
    return term if total is None else total + term


def slab_copy(span, n, matrix_ref, target_ref, sems):
    _, height, width = target_ref.shape
    unit = height // span[1]
    return pltpu.make_async_copy(
        matrix_ref.at[
            pl.ds(span[0] * unit, height),
            pl.ds(n * width if isinstance(n, int) else pl.multiple_of(n * width, width), width),
        ],
        target_ref.at[n],
        sems.at[n],
    )


def slab_scores(n, rows_ref, chunk, parts, stream, matrix_ref, stream_ref, sems, total):
    width = stream_ref.shape[2]
    start = n * width if isinstance(n, int) else pl.multiple_of(n * width, width)
    cols = pl.ds(start, width)
    if not isinstance(n, int):
        slab_copy(stream, n, matrix_ref, stream_ref, sems).wait()
    for weight_ref, span in parts:
        total = product(rows_ref, chunk, weight_ref, span, cols, total)
    if isinstance(n, int):
        slab_copy(stream, n, matrix_ref, stream_ref, sems).wait()
    return product(rows_ref, chunk, stream_ref.at[n], stream, slice(None), total)


def partial_kernel(rows_ref, *refs, spans, beside):
    weight_refs, refs = refs[: len(spans)], refs[len(spans) :]
    matrix_ref, out_ref, fetched_ref, sems = refs
    copies = unit_copies(beside, matrix_ref, fetched_ref, sems)
    for copy in copies:
        copy.start()
    width = min(SLAB, out_ref.shape[1])

    def step(n, carry):
        cols = pl.ds(pl.multiple_of(n * width, width), width)
        total = None
        for weight_ref, span in zip(weight_refs, spans):
            total = product(rows_ref, 0, weight_ref, span, cols, total)
        out_ref[:, cols] = total
        return carry

    lax.fori_loop(0, out_ref.shape[1] // width, step, 0)
    for copy in copies:
        copy.wait()


def slabs_shape(span, matrix, width):
    features, cols = matrix.shape
    width = min(width, cols)
    return pltpu.VMEM((cols // width, features // UNITS * span[1], width), matrix.dtype)


def partial_scores(rows, weights, spans, matrix, beside):
    groups, group_rows, _ = rows.shape
    return pl.pallas_call(
        functools.partial(partial_kernel, spans=spans, beside=beside),
        out_shape=(
            pltpu.VMEM((groups * group_rows, matrix.shape[1]), jnp.float32),
            rows_shape(beside, matrix),
        ),
        in_specs=[VMEM] * (1 + len(weights)) + [ANY],
        out_specs=(VMEM, VMEM),
        scratch_shapes=[pltpu.SemaphoreType.DMA((beside[1],))],
        compiler_params=pltpu.CompilerParams(vmem_limit_bytes=2 * MIB),
        cost_estimate=pl.CostEstimate(flops=10**11, bytes_accessed=0, transcendentals=0),
        name="partial",
    )(rows, *weights, matrix)


def final_kernel(rows_ref, *refs, spans, late, batch_offsets, batch_count):
    early_refs, refs = refs[: len(spans)], refs[len(spans) :]
    (scores_ref, heat_ref, choice_ref, ids_ref, matrix_ref, keep_ref, send_ref) = refs[:7]
    late_ref, temp_ref, local_ids_ref, cand_ref, top_ref, total_ref, held_ref, sems = refs[7:]
    cols = scores_ref.shape[1]
    group_rows = rows_ref.shape[1]
    vocab_pos = lax.axis_index("vocab")
    batch_pos = lax.axis_index("batch")
    offset = (vocab_pos * batch_count + batch_pos) * cols
    slabs, _, width = late_ref.shape
    for n in range(slabs):
        slab_copy(late, n, matrix_ref, late_ref, sems).start()

    for s, j in enumerate(batch_offsets):
        rows = pl.ds(s * group_rows, group_rows)
        for row in range(group_rows):
            heat = heat_ref[choice_ref[(batch_pos ^ j) * group_rows + row]]
            temp_ref[pl.ds(s * group_rows + row, 1), :] = jnp.full((1, LANES), heat, jnp.float32)
        local_ids_ref[rows, :] = ids_ref[batch_pos ^ j] - offset
    cand_ref[...] = jnp.zeros_like(cand_ref)
    top_ref[...] = jnp.full_like(top_ref, -3e38)
    total_ref[...] = jnp.zeros_like(total_ref)

    parts = list(zip(early_refs, spans))

    def scores_of(n):
        at = n * width if isinstance(n, int) else pl.multiple_of(n * width, width)
        before = scores_ref[:, pl.ds(at, width)]
        return slab_scores(
            n, rows_ref, CHUNKS - 1, parts, late, matrix_ref, late_ref, sems, before
        )

    def count_in(n):
        scores = held_ref[n & 1]
        temp = temp_ref[...]
        local_ids = local_ids_ref[...]
        lane = local_ids & (LANES - 1)
        chunk_of = local_ids >> (LANES.bit_length() - 1)
        cand = cand_ref[...]
        chunks = []
        for c in range(width // LANES):
            scaled = scores[:, c * LANES : (c + 1) * LANES] / temp
            chunks.append(scaled)
            picked = jnp.take_along_axis(scaled, lane, axis=1, mode="promise_in_bounds")
            cand = jnp.where(chunk_of == n * (width // LANES) + c, picked, cand)
        cand_ref[...] = cand
        top = top_ref[...]
        new_top = functools.reduce(jnp.maximum, chunks, top)
        total = total_ref[...] * jnp.exp(top - new_top)
        for scaled in chunks:
            total = total + jnp.exp(scaled - new_top)
        top_ref[...] = new_top
        total_ref[...] = total

    held_ref[0] = scores_of(0)

    def step(n, carry):
        scores = scores_of(n)
        count_in(n - 1)
        held_ref[n & 1] = scores
        return carry

    lax.fori_loop(1, slabs, step, 0)
    count_in(slabs - 1)

    top = top_ref[...]
    row_top = jnp.max(top, axis=1, keepdims=True)
    row_total = jnp.sum(total_ref[...] * jnp.exp(top - row_top), axis=1, keepdims=True)
    row_log = jnp.broadcast_to(row_top + jnp.log(row_total), top.shape)
    for s, j in enumerate(batch_offsets):
        out_ref = send_ref if j & 1 else keep_ref
        out_ref[0, j // 2] = cand_ref[pl.ds(s * group_rows, group_rows), :]
        out_ref[1, j // 2] = row_log[s * group_rows : (s + 1) * group_rows]


def final(rows, early, spans, late, scores, heat, choice, ids, matrix, batch_offsets):
    batch_count, group_rows, _ = rows.shape
    slots, _ = scores.shape
    half = jax.ShapeDtypeStruct((2, batch_count // 2, group_rows, LANES), jnp.float32)
    rows_f32 = pltpu.VMEM((slots, LANES), jnp.float32)
    slabs = slabs_shape(late, matrix, 512)
    body = functools.partial(
        final_kernel, spans=spans, late=late, batch_offsets=batch_offsets, batch_count=batch_count
    )
    return pl.pallas_call(
        body,
        out_shape=(half, half),
        in_specs=[VMEM] * (len(early) + 2) + [SMEM, SMEM, VMEM, ANY],
        out_specs=(VMEM, VMEM),
        scratch_shapes=[
            slabs,
            rows_f32,
            pltpu.VMEM((slots, LANES), jnp.int32),
            rows_f32,
            rows_f32,
            rows_f32,
            pltpu.VMEM((2, slots, slabs.shape[2]), jnp.float32),
            pltpu.SemaphoreType.DMA((slabs.shape[0],)),
        ],
        compiler_params=pltpu.CompilerParams(
            vmem_limit_bytes=matrix.size // UNITS * late[1] * 2 + 3 * MIB
        ),
        name="final",
    )(rows, *early, scores, heat, choice, ids, matrix)


def joined(values):
    plane = lax.broadcasted_iota(jnp.int32, values[0].shape, 0)
    high = functools.reduce(jnp.maximum, values)
    total = sum(jnp.exp(value - high) for value in values)
    return jnp.where(plane == 0, sum(values), high + jnp.log(total))


def finish_kernel(keep_ref, *refs):
    *value_refs, log_ref, mass_ref, weights_ref, keep_rows_ref = refs
    group_rows, count = weights_ref.shape
    first = lax.axis_index("batch") * group_rows
    for row in range(group_rows):
        keep_rows_ref[pl.ds(row, 1), :] = jnp.full((1, count), keep_ref[first + row], jnp.int32)
    cand = sum(ref[0, 0] for ref in value_refs)
    logs = [ref[1, 0] for ref in value_refs]
    high = functools.reduce(jnp.maximum, logs)
    log_norm = high + jnp.log(sum(jnp.exp(value - high) for value in logs))
    lane = lax.broadcasted_iota(jnp.int32, (group_rows, count), 1)
    kept = lane < keep_rows_ref[...]
    top = jnp.max(jnp.where(kept, cand, jnp.float32(-3e38)), axis=1, keepdims=True)
    kept_exp = jnp.where(kept, jnp.exp(jnp.where(kept, cand - top, 0.0)), 0.0)
    kept_sum = jnp.sum(kept_exp, axis=1, keepdims=True)
    weights_ref[...] = kept_exp / kept_sum
    mass = jnp.broadcast_to(top + jnp.log(kept_sum), log_norm.shape) - log_norm
    own = lane == lax.broadcasted_iota(jnp.int32, lane.shape, 0)
    for ref, value in ((log_ref, log_norm), (mass_ref, mass)):
        row = jnp.sum(jnp.where(own, value, 0.0), axis=0, keepdims=True)
        ref[...] = row[:, :group_rows]


def finish(keep_count, values):
    group_rows, count = values[0].shape[2:]
    row = jax.ShapeDtypeStruct((1, group_rows), jnp.float32)
    log_norm, mass, weights = pl.pallas_call(
        finish_kernel,
        out_shape=(row, row, jax.ShapeDtypeStruct((group_rows, count), jnp.float32)),
        in_specs=[SMEM] + [VMEM] * len(values),
        out_specs=(VMEM,) * 3,
        scratch_shapes=[pltpu.VMEM((group_rows, count), jnp.int32)],
        compiler_params=pltpu.CompilerParams(vmem_limit_bytes=MIB),
        name="finish",
    )(keep_count, *values)
    return log_norm.reshape(-1), mass.reshape(-1), weights


def local(
    latent_state_rows,
    closing_rescale_coeffs,
    output_projection_matrix,
    config_heat_values,
    sequence_config_choice,
    ranked_choice_ids,
    keep_count,
):
    group_rows, _ = latent_state_rows.shape
    matrix = output_projection_matrix
    vocab_count = lax.axis_size("vocab")
    batch_count = lax.axis_size("batch")
    vocab_rounds = rounds_of(bits_of(vocab_count))
    vocab_bits = sum(vocab_rounds, [])
    batch_bits = bits_of(batch_count)[::-1]
    offsets = offsets_of(vocab_bits)
    batch_offsets = offsets_of(batch_bits)

    fetched, spans = [], []

    def fetch_next(after=None):
        span = (sum(spans[-1]) if spans else 0, EARLY_UNITS[len(spans)])
        spans.append(span)
        fetched.append(fetch(span, matrix, after))

    blocks = latent_state_rows[None]
    for n, bits in enumerate(vocab_rounds):
        others = []
        for offset in offsets_of(bits)[1:]:
            others.append(swap(blocks, "vocab", offset))
        if n < 2:
            fetch_next(blocks if n else None)
        blocks = jnp.concatenate([blocks, *others], axis=0)
    chunks = list(norm(blocks, closing_rescale_coeffs, offsets))
    for n, bit in enumerate(batch_bits):
        others = []
        for chunk in chunks:
            others.append(swap(chunk, "batch", bit))
        if n < 2:
            fetch_next(chunks[0])
        chunks = [jnp.concatenate(pair, axis=0) for pair in zip(chunks, others)]
    border = UNITS // CHUNKS
    mine = [n for n, span in enumerate(spans) if span[0] < border]
    beside = (sum(spans[-1]), BESIDE_UNITS)
    scores, extra = partial_scores(
        chunks[0], [fetched[n] for n in mine], [spans[n] for n in mine], matrix, beside
    )
    fetched.append(extra)
    spans.append(beside)
    late = (sum(beside), UNITS - sum(beside))
    rest = [n for n, span in enumerate(spans) if sum(span) > border]
    kept, sent = final(
        chunks[1],
        [fetched[n] for n in rest],
        [spans[n] for n in rest],
        late,
        scores,
        config_heat_values,
        sequence_config_choice,
        ranked_choice_ids.reshape(batch_count, group_rows, -1),
        matrix,
        batch_offsets,
    )
    kept = joined([kept, swap(sent, "batch", 1)])
    *vocab_rounds, near = vocab_rounds
    for bit in bits_of(batch_count)[1:]:
        half = [kept[:, 0::2], kept[:, 1::2]]
        values = [half[0], swap(half[1], "batch", bit)]
        if near:
            offset = near.pop()
            values += [swap(half[0], "vocab", offset), swap_both(half[1], offset, bit)]
        kept = joined(values)
    last = [kept]
    for bits in vocab_rounds[::-1] + [near]:
        if bits:
            kept = joined(last) if len(last) > 1 else kept
            last = [kept] + [swap(kept, "vocab", m) for m in offsets_of(bits)[:0:-1]]
    return finish(keep_count, last)


def solution(mesh):
    placed = (P("batch", "vocab"), P(), P(None, ("vocab", "batch")), P(), P(), P(), P())
    return jax.shard_map(
        local,
        mesh=mesh,
        in_specs=placed,
        out_specs=(P("batch"), P("batch"), P("batch", None)),
        check_vma=False,
    )
```

```python
import functools

import jax
import jax.numpy as jnp
from jax import lax
from jax.experimental import pallas as pl
from jax.experimental.pallas import tpu as pltpu
from jax.sharding import PartitionSpec as P


epsilon = 1e-06
LANES = 128
UNITS = 32
CHUNKS = 2
EARLY_UNITS = (6, 4, 5, 1)
BESIDE_UNITS = 7
MIB = 1 << 20
SLAB = 2048


VMEM = pl.BlockSpec(memory_space=pltpu.VMEM)
SMEM = pl.BlockSpec(memory_space=pltpu.SMEM)
ANY = pl.BlockSpec(memory_space=pl.ANY)


def bits_of(count):
    return [1 << n for n in range(count.bit_length() - 1)]


def swap(value, axis, bit):
    count = lax.axis_size(axis)
    return lax.ppermute(value, axis, [(n, n ^ bit) for n in range(count)])


def swap_both(value, vocab_offset, batch_offset):
    vocab_count = lax.axis_size("vocab")
    batch_count = lax.axis_size("batch")
    pairs = [
        (v * batch_count + b, (v ^ vocab_offset) * batch_count + (b ^ batch_offset))
        for v in range(vocab_count)
        for b in range(batch_count)
    ]
    return lax.ppermute(value, ("vocab", "batch"), pairs)


def rounds_of(bits):
    bits = sorted(bits, reverse=True)
    return [bits[n : n + 2] for n in range(0, len(bits), 2)]


def offsets_of(bits):
    offsets = [0]
    for bit in bits:
        offsets += [offset ^ bit for offset in offsets]
    return offsets


def unit_copies(span, matrix_ref, target_ref, sems):
    first, count = span
    height = target_ref.shape[0] // count
    return [
        pltpu.make_async_copy(
            matrix_ref.at[pl.ds((first + n) * height, height)],
            target_ref.at[pl.ds(n * height, height)],
            sems.at[n],
        )
        for n in range(count)
    ]


def fetch_kernel(*refs, span):
    matrix_ref, out_ref, sems = refs[-3:]
    copies = unit_copies(span, matrix_ref, out_ref, sems)
    for copy in copies:
        copy.start()
    for copy in copies:
        copy.wait()


def rows_shape(span, matrix):
    features, cols = matrix.shape
    return pltpu.VMEM((features // UNITS * span[1], cols), matrix.dtype)


def fetch(span, matrix, after=None):
    operands = [matrix] if after is None else [after, matrix]
    return pl.pallas_call(
        functools.partial(fetch_kernel, span=span),
        out_shape=rows_shape(span, matrix),
        in_specs=[ANY] * len(operands),
        out_specs=VMEM,
        scratch_shapes=[pltpu.SemaphoreType.DMA((span[1],))],
        compiler_params=pltpu.CompilerParams(vmem_limit_bytes=MIB),
        cost_estimate=pl.CostEstimate(
            flops=span[1] * 10**10, bytes_accessed=matrix.size * 2 // UNITS * span[1], transcendentals=0
        ),
    )(*operands)


def table_fetch_kernel(
    after_ref, heat_ref, choice_ref, keep_ref, ids_ref, matrix_ref, *refs, span, order
):
    out_ref, temp_ref, local_ids_ref, keep_rows_ref, sems = refs
    copies = unit_copies(span, matrix_ref, out_ref, sems)
    for copy in copies:
        copy.start()
    group_rows = keep_rows_ref.shape[0]
    batch_pos = lax.axis_index("batch")
    place = lax.axis_index("vocab") * lax.axis_size("batch") + batch_pos
    for s, j in enumerate(order):
        first = (batch_pos ^ j) * group_rows
        rows = pl.ds(s * group_rows, group_rows)
        local_ids_ref[rows, :] = ids_ref[batch_pos ^ j] - place * matrix_ref.shape[1]
        for row in range(group_rows):
            heat = heat_ref[choice_ref[first + row]]
            temp_ref[pl.ds(s * group_rows + row, 1), :] = jnp.full((1, LANES), heat, jnp.float32)
    for row in range(group_rows):
        keep = keep_ref[batch_pos * group_rows + row]
        keep_rows_ref[pl.ds(row, 1), :] = jnp.full((1, LANES), keep, jnp.int32)
    for copy in copies:
        copy.wait()


def table_fetch(span, after, heat, choice, keep, ids, matrix, order):
    groups, group_rows, _ = ids.shape
    slots = groups * group_rows
    return pl.pallas_call(
        functools.partial(table_fetch_kernel, span=span, order=order),
        out_shape=(
            rows_shape(span, matrix),
            jax.ShapeDtypeStruct((slots, LANES), jnp.float32),
            jax.ShapeDtypeStruct((slots, LANES), jnp.int32),
            jax.ShapeDtypeStruct((group_rows, LANES), jnp.int32),
        ),
        in_specs=[ANY, SMEM, SMEM, SMEM, VMEM, ANY],
        out_specs=(VMEM,) * 4,
        scratch_shapes=[pltpu.SemaphoreType.DMA((span[1],))],
        compiler_params=pltpu.CompilerParams(vmem_limit_bytes=MIB),
        cost_estimate=pl.CostEstimate(flops=10**11, bytes_accessed=0, transcendentals=0),
        name="tables",
    )(after, heat, choice, keep, ids, matrix)


def norm_kernel(pieces_ref, gain_ref, *out_refs, offsets):
    vocab_pos = lax.axis_index("vocab")
    count, group_rows, part = pieces_ref.shape
    per_chunk = count // CHUNKS
    order_bits = [offsets[1 << n] for n in range(count.bit_length() - 1)]
    square = jnp.zeros((group_rows, part), jnp.float32)
    for n in range(count):
        values = pieces_ref[n].astype(jnp.float32)
        square = square + values * values
    factor = lax.rsqrt(jnp.sum(square, axis=1, keepdims=True) / (count * part) + epsilon)
    for n in range(count):
        apart = vocab_pos ^ n
        place = sum(
            ((apart >> (bit.bit_length() - 1)) & 1) << k for k, bit in enumerate(order_bits)
        )
        values = pieces_ref[place].astype(jnp.float32)
        gain = gain_ref[n * part : (n + 1) * part].astype(jnp.float32).reshape(1, part)
        out_refs[n // per_chunk][0, :, pl.ds(n % per_chunk * part, part)] = (
            values * factor * gain
        ).astype(jnp.bfloat16)


def norm(pieces, gain, offsets):
    count, group_rows, part = pieces.shape
    chunk = jax.ShapeDtypeStruct((1, group_rows, count * part // CHUNKS), jnp.bfloat16)
    return pl.pallas_call(
        functools.partial(norm_kernel, offsets=offsets),
        out_shape=(chunk,) * CHUNKS,
        in_specs=[VMEM, VMEM],
        out_specs=(VMEM,) * CHUNKS,
        compiler_params=pltpu.CompilerParams(vmem_limit_bytes=4 * MIB),
        name="norm",
    )(pieces, gain)


def product(rows_ref, chunk, weight_ref, span, cols, total=None):
    groups, group_rows, width = rows_ref.shape
    per_chunk = UNITS // CHUNKS
    unit = width // per_chunk
    low = max(span[0], chunk * per_chunk)
    high = min(span[0] + span[1], (chunk + 1) * per_chunk)
    if low >= high:
        return total
    rows = rows_ref[
        :, :, (low - chunk * per_chunk) * unit : (high - chunk * per_chunk) * unit
    ].reshape(groups * group_rows, (high - low) * unit)
    weights = weight_ref[(low - span[0]) * unit : (high - span[0]) * unit, cols]
    term = jnp.dot(rows, weights, preferred_element_type=jnp.float32)
    return term if total is None else total + term


def slab_copy(span, n, matrix_ref, target_ref, sems):
    _, height, width = target_ref.shape
    unit = height // span[1]
    return pltpu.make_async_copy(
        matrix_ref.at[
            pl.ds(span[0] * unit, height),
            pl.ds(n * width if isinstance(n, int) else pl.multiple_of(n * width, width), width),
        ],
        target_ref.at[n],
        sems.at[n],
    )


def slab_scores(n, rows_ref, chunk, parts, stream, matrix_ref, stream_ref, sems, total):
    width = stream_ref.shape[2]
    start = n * width if isinstance(n, int) else pl.multiple_of(n * width, width)
    cols = pl.ds(start, width)
    if not isinstance(n, int):
        slab_copy(stream, n, matrix_ref, stream_ref, sems).wait()
    for weight_ref, span in parts:
        total = product(rows_ref, chunk, weight_ref, span, cols, total)
    if isinstance(n, int):
        slab_copy(stream, n, matrix_ref, stream_ref, sems).wait()
    return product(rows_ref, chunk, stream_ref.at[n], stream, slice(None), total)


def partial_kernel(rows_ref, *refs, spans, beside):
    weight_refs, refs = refs[: len(spans)], refs[len(spans) :]
    matrix_ref, out_ref, fetched_ref, sems = refs
    copies = unit_copies(beside, matrix_ref, fetched_ref, sems)
    for copy in copies:
        copy.start()
    width = min(SLAB, out_ref.shape[1])

    def step(n, carry):
        cols = pl.ds(pl.multiple_of(n * width, width), width)
        total = None
        for weight_ref, span in zip(weight_refs, spans):
            total = product(rows_ref, 0, weight_ref, span, cols, total)
        out_ref[:, cols] = total
        return carry

    lax.fori_loop(0, out_ref.shape[1] // width, step, 0)
    for copy in copies:
        copy.wait()


def slabs_shape(span, matrix, width):
    features, cols = matrix.shape
    width = min(width, cols)
    return pltpu.VMEM((cols // width, features // UNITS * span[1], width), matrix.dtype)


def partial_scores(rows, weights, spans, matrix, beside):
    groups, group_rows, _ = rows.shape
    return pl.pallas_call(
        functools.partial(partial_kernel, spans=spans, beside=beside),
        out_shape=(
            pltpu.VMEM((groups * group_rows, matrix.shape[1]), jnp.float32),
            rows_shape(beside, matrix),
        ),
        in_specs=[VMEM] * (1 + len(weights)) + [ANY],
        out_specs=(VMEM, VMEM),
        scratch_shapes=[pltpu.SemaphoreType.DMA((beside[1],))],
        compiler_params=pltpu.CompilerParams(vmem_limit_bytes=2 * MIB),
        cost_estimate=pl.CostEstimate(flops=10**11, bytes_accessed=0, transcendentals=0),
        name="partial",
    )(rows, *weights, matrix)


def final_kernel(
    rows_ref, *refs, spans, late, batch_offsets
):
    early_refs, refs = refs[: len(spans)], refs[len(spans) :]
    (scores_ref, temp_ref, local_ids_ref, matrix_ref, keep_ref, send_ref) = refs[:6]
    late_ref, cand_ref, top_ref, total_ref, held_ref, sems = refs[6:]
    group_rows = rows_ref.shape[1]
    slabs, _, width = late_ref.shape
    for n in range(slabs):
        slab_copy(late, n, matrix_ref, late_ref, sems).start()

    cand_ref[...] = jnp.zeros_like(cand_ref)
    top_ref[...] = jnp.full_like(top_ref, -3e38)
    total_ref[...] = jnp.zeros_like(total_ref)

    parts = list(zip(early_refs, spans))

    def scores_of(n):
        at = n * width if isinstance(n, int) else pl.multiple_of(n * width, width)
        before = scores_ref[:, pl.ds(at, width)]
        return slab_scores(
            n, rows_ref, CHUNKS - 1, parts, late, matrix_ref, late_ref, sems, before
        )

    def count_in(n):
        scores = held_ref[n & 1]
        temp = temp_ref[...]
        local_ids = local_ids_ref[...]
        lane = local_ids & (LANES - 1)
        chunk_of = local_ids >> (LANES.bit_length() - 1)
        cand = cand_ref[...]
        chunks = []
        for c in range(width // LANES):
            scaled = scores[:, c * LANES : (c + 1) * LANES] / temp
            chunks.append(scaled)
            picked = jnp.take_along_axis(scaled, lane, axis=1, mode="promise_in_bounds")
            cand = jnp.where(chunk_of == n * (width // LANES) + c, picked, cand)
        cand_ref[...] = cand
        top = top_ref[...]
        new_top = functools.reduce(jnp.maximum, chunks, top)
        total = total_ref[...] * jnp.exp(top - new_top)
        for scaled in chunks:
            total = total + jnp.exp(scaled - new_top)
        top_ref[...] = new_top
        total_ref[...] = total

    held_ref[0] = scores_of(0)

    def step(n, carry):
        scores = scores_of(n)
        count_in(n - 1)
        held_ref[n & 1] = scores
        return carry

    lax.fori_loop(1, slabs, step, 0)
    count_in(slabs - 1)

    top = top_ref[...]
    row_top = jnp.max(top, axis=1, keepdims=True)
    row_total = jnp.sum(total_ref[...] * jnp.exp(top - row_top), axis=1, keepdims=True)
    row_log = jnp.broadcast_to(row_top + jnp.log(row_total), top.shape)
    for s, j in enumerate(batch_offsets):
        out_ref = send_ref if j & 1 else keep_ref
        out_ref[0, j // 2] = cand_ref[pl.ds(s * group_rows, group_rows), :]
        out_ref[1, j // 2] = row_log[s * group_rows : (s + 1) * group_rows]


def final(rows, early, spans, late, scores, temp, local_ids, matrix, batch_offsets):
    batch_count, group_rows, _ = rows.shape
    slots, _ = scores.shape
    half = jax.ShapeDtypeStruct((2, batch_count // 2, group_rows, LANES), jnp.float32)
    rows_f32 = pltpu.VMEM((slots, LANES), jnp.float32)
    slabs = slabs_shape(late, matrix, 512)
    body = functools.partial(
        final_kernel,
        spans=spans,
        late=late,
        batch_offsets=batch_offsets,
    )
    return pl.pallas_call(
        body,
        out_shape=(half, half),
        in_specs=[VMEM] * (len(early) + 4) + [ANY],
        out_specs=(VMEM, VMEM),
        scratch_shapes=[
            slabs,
            rows_f32,
            rows_f32,
            rows_f32,
            pltpu.VMEM((2, slots, slabs.shape[2]), jnp.float32),
            pltpu.SemaphoreType.DMA((slabs.shape[0],)),
        ],
        compiler_params=pltpu.CompilerParams(
            vmem_limit_bytes=matrix.size // UNITS * late[1] * 2 + 3 * MIB
        ),
        name="final",
    )(rows, *early, scores, temp, local_ids, matrix)


def joined(values):
    plane = lax.broadcasted_iota(jnp.int32, values[0].shape, 0)
    high = functools.reduce(jnp.maximum, values)
    total = sum(jnp.exp(value - high) for value in values)
    return jnp.where(plane == 0, sum(values), high + jnp.log(total))


def finish_kernel(keep_rows_ref, *refs):
    *value_refs, log_ref, mass_ref, weights_ref = refs
    group_rows, count = weights_ref.shape
    cand = sum(ref[0, 0] for ref in value_refs)
    logs = [ref[1, 0] for ref in value_refs]
    high = functools.reduce(jnp.maximum, logs)
    log_norm = high + jnp.log(sum(jnp.exp(value - high) for value in logs))
    lane = lax.broadcasted_iota(jnp.int32, (group_rows, count), 1)
    kept = lane < keep_rows_ref[...]
    top = jnp.max(jnp.where(kept, cand, jnp.float32(-3e38)), axis=1, keepdims=True)
    kept_exp = jnp.where(kept, jnp.exp(jnp.where(kept, cand - top, 0.0)), 0.0)
    kept_sum = jnp.sum(kept_exp, axis=1, keepdims=True)
    weights_ref[...] = kept_exp / kept_sum
    mass = jnp.broadcast_to(top + jnp.log(kept_sum), log_norm.shape) - log_norm
    own = lane == lax.broadcasted_iota(jnp.int32, lane.shape, 0)
    for ref, value in ((log_ref, log_norm), (mass_ref, mass)):
        row = jnp.sum(jnp.where(own, value, 0.0), axis=0, keepdims=True)
        ref[...] = row[:, :group_rows]


def finish(keep_rows, values):
    group_rows, count = values[0].shape[2:]
    row = jax.ShapeDtypeStruct((1, group_rows), jnp.float32)
    log_norm, mass, weights = pl.pallas_call(
        finish_kernel,
        out_shape=(row, row, jax.ShapeDtypeStruct((group_rows, count), jnp.float32)),
        in_specs=[VMEM] * (1 + len(values)),
        out_specs=(VMEM,) * 3,
        compiler_params=pltpu.CompilerParams(vmem_limit_bytes=MIB),
        name="finish",
    )(keep_rows, *values)
    return log_norm.reshape(-1), mass.reshape(-1), weights


def local(
    latent_state_rows,
    closing_rescale_coeffs,
    output_projection_matrix,
    config_heat_values,
    sequence_config_choice,
    ranked_choice_ids,
    keep_count,
):
    group_rows, _ = latent_state_rows.shape
    matrix = output_projection_matrix
    vocab_count = lax.axis_size("vocab")
    batch_count = lax.axis_size("batch")
    vocab_rounds = rounds_of(bits_of(vocab_count))
    vocab_bits = sum(vocab_rounds, [])
    batch_bits = bits_of(batch_count)[::-1]
    offsets = offsets_of(vocab_bits)
    batch_offsets = offsets_of(batch_bits)

    fetched, spans = [], []

    def fetch_next(after=None):
        span = (sum(spans[-1]) if spans else 0, EARLY_UNITS[len(spans)])
        spans.append(span)
        fetched.append(fetch(span, matrix, after))

    blocks = latent_state_rows[None]
    for n, bits in enumerate(vocab_rounds):
        others = []
        for offset in offsets_of(bits)[1:]:
            others.append(swap(blocks, "vocab", offset))
        if n < 2:
            fetch_next(blocks if n else None)
        blocks = jnp.concatenate([blocks, *others], axis=0)
    chunks = list(norm(blocks, closing_rescale_coeffs, offsets))
    for n, bit in enumerate(batch_bits):
        others = []
        for chunk in chunks:
            others.append(swap(chunk, "batch", bit))
        if n == 0:
            spans.append((sum(spans[-1]), EARLY_UNITS[2]))
            weights, temp, local_ids, keep_rows = table_fetch(
                spans[-1],
                chunks[0],
                config_heat_values,
                sequence_config_choice,
                keep_count,
                ranked_choice_ids.reshape(batch_count, group_rows, -1),
                matrix,
                batch_offsets,
            )
            fetched.append(weights)
        elif n == 1:
            fetch_next(chunks[0])
        chunks = [jnp.concatenate(pair, axis=0) for pair in zip(chunks, others)]
    border = UNITS // CHUNKS
    mine = [n for n, span in enumerate(spans) if span[0] < border]
    beside = (sum(spans[-1]), BESIDE_UNITS)
    scores, extra = partial_scores(
        chunks[0], [fetched[n] for n in mine], [spans[n] for n in mine], matrix, beside
    )
    fetched.append(extra)
    spans.append(beside)
    late = (sum(beside), UNITS - sum(beside))
    rest = [n for n, span in enumerate(spans) if sum(span) > border]
    kept, sent = final(
        chunks[1],
        [fetched[n] for n in rest],
        [spans[n] for n in rest],
        late,
        scores,
        temp,
        local_ids,
        matrix,
        batch_offsets,
    )
    kept = joined([kept, swap(sent, "batch", 1)])
    *vocab_rounds, near = vocab_rounds
    for bit in bits_of(batch_count)[1:]:
        half = [kept[:, 0::2], kept[:, 1::2]]
        values = [half[0], swap(half[1], "batch", bit)]
        if near:
            offset = near.pop()
            values += [swap(half[0], "vocab", offset), swap_both(half[1], offset, bit)]
        kept = joined(values)
    last = [kept]
    for bits in vocab_rounds[::-1] + [near]:
        if bits:
            kept = joined(last) if len(last) > 1 else kept
            last = [kept] + [swap(kept, "vocab", m) for m in offsets_of(bits)[:0:-1]]
    return finish(keep_rows, last)


def solution(mesh):
    placed = (P("batch", "vocab"), P(), P(None, ("vocab", "batch")), P(), P(), P(), P())
    return jax.shard_map(
        local,
        mesh=mesh,
        in_specs=placed,
        out_specs=(P("batch"), P("batch"), P("batch", None)),
        check_vma=False,
    )
```
